32 devices in a mesh: rad: 8 (over y, x, core), ang: 4 (over z).
Axes of the slice: x: 2, y: 2, z: 4, core: 2. Of those that a mesh axis runs over, the one named last changes fastest.
Arguments:
- density: float32 [3, 512, 128, 512], P(None, 'rad', 'ang'), may hold values from -13 to 13
Outputs:
- potential: float32 [3, 512, 128, 512], P(None, 'rad', 'ang')
The draws below stay inside these ranges and needn't reach their ends.
All inputs are finite; a program needn't handle non-finite values.
Results may differ from the reference program's by a relative error of at most 0.0003.
Values sent between devices are 32-bit elements; how exact they have to be, the bound alone decides.
A program may use at most 128 MiB of HBM per device.

```python
import math
import jax
import jax.numpy as jnp
from jax import lax

LMAX = 12
NPHI = 512
FIELDS = 3
NR = 512
NTH = 128


def draw_density(key, part):
    key_scale, key_noise = jax.random.split(jax.random.fold_in(key, 11))
    scales = jnp.exp(jax.random.uniform(key_scale, (FIELDS, NR, 1, 1), jnp.float32, math.log(0.5), math.log(2.0)))
    noise = jax.random.truncated_normal(key_noise, -3.0, 3.0, (FIELDS, NR, NTH, NPHI), jnp.float32)
    rough = (noise - jnp.roll(noise, 1, axis=1)) * math.sqrt(0.5)
    return scales * rough


def setup_inputs(seed: int = 0) -> dict:
    arg_keys = jax.random.split(jax.random.key(seed), 2)
    return {
        "density": draw_density(jax.random.fold_in(arg_keys[1], 71), 0),
    }


INNER = 0.5
COUPLING = 2000.0

def legendre_table(polar_angle):
    cos_theta = jnp.cos(polar_angle)
    sine_theta = jnp.sin(polar_angle)
    values_lm = {}
    values_lm[0, 0] = jnp.full_like(polar_angle, 1.0 / math.sqrt(4.0 * math.pi))
    for m in range(1, LMAX + 1):
        values_lm[m, m] = math.sqrt((2.0 * m + 1.0) / (2.0 * m)) * sine_theta * values_lm[m - 1, m - 1]
    for m in range(0, LMAX):
        values_lm[m + 1, m] = math.sqrt(2.0 * m + 3.0) * cos_theta * values_lm[m, m]
    for m in range(0, LMAX + 1):
        for l in range(m + 2, LMAX + 1):
            coef_a = math.sqrt((4.0 * l * l - 1.0) / (l * l - m * m))
            coef_b = math.sqrt(((l - 1.0) ** 2 - m * m) / (4.0 * (l - 1.0) ** 2 - 1.0))
            values_lm[l, m] = coef_a * (cos_theta * values_lm[l - 1, m] - coef_b * values_lm[l - 2, m])
    degree_rows = []
    for l in range(LMAX + 1):
        columns = []
        for k in range(2 * LMAX + 1):
            m = (k + 1) // 2
            columns.append(values_lm[l, m] if m <= l else jnp.zeros_like(polar_angle))
        degree_rows.append(jnp.stack(columns, -1))
    return jnp.stack(degree_rows, 1)

def fourier_table(phi_cells):
    azimuth = jnp.arange(phi_cells, dtype=jnp.float32) * (2.0 * math.pi / phi_cells)
    column = jnp.arange(2 * LMAX + 1)
    order_m = ((column + 1) // 2).astype(jnp.float32)
    phase = azimuth[:, None] * order_m[None, :]
    root_two = math.sqrt(2.0)
    return jnp.where(column[None, :] == 0, jnp.ones_like(phase), jnp.where(column[None, :] % 2 == 1, root_two * jnp.cos(phase), root_two * jnp.sin(phase)))

def one_field(density):
    shells, theta_rows, phi_cells = density.shape
    polar_angle = (jnp.arange(theta_rows, dtype=jnp.float32) + 0.5) * (math.pi / theta_rows)
    legendre = legendre_table(polar_angle)
    weights = jnp.sin(polar_angle) * (math.pi / theta_rows) * (2.0 * math.pi / phi_cells)
    fourier = fourier_table(phi_cells)
    spacing = (1.0 - INNER) / shells
    radius = INNER + (jnp.arange(shells, dtype=jnp.float32) + 0.5) * spacing
    azimuthal = jnp.dot(density.reshape(shells * theta_rows, phi_cells), fourier, precision=lax.Precision.HIGHEST, preferred_element_type=jnp.float32)
    azimuthal = azimuthal.reshape(shells, theta_rows, 2 * LMAX + 1)
    moments = jnp.einsum('rtk,tlk->rlk', azimuthal, legendre * weights[:, None, None], precision=lax.Precision.HIGHEST)
    degree = jnp.arange(LMAX + 1, dtype=jnp.float32)
    inner_terms = moments * (radius[:, None] ** (degree + 2.0) * spacing)[:, :, None]
    outer_terms = moments * (radius[:, None] ** (1.0 - degree) * spacing)[:, :, None]
    inner_sum = jnp.cumsum(inner_terms, 0) - 0.5 * inner_terms
    outer_sum = jnp.flip(jnp.cumsum(jnp.flip(outer_terms, 0), 0), 0) - 0.5 * outer_terms
    factor = (-COUPLING * 4.0 * math.pi / (2.0 * degree + 1.0))[None, :, None]
    coefficient = factor * (radius[:, None, None] ** (-(degree[None, :, None] + 1.0)) * inner_sum + radius[:, None, None] ** degree[None, :, None] * outer_sum)
    spread = jnp.einsum('rlk,tlk->rtk', coefficient, legendre, precision=lax.Precision.HIGHEST)
    potential = jnp.dot(spread.reshape(shells * theta_rows, 2 * LMAX + 1), fourier.T, precision=lax.Precision.HIGHEST, preferred_element_type=jnp.float32)
    return potential.reshape(shells, theta_rows, phi_cells)

def reference(density):
    return lax.map(one_field, density)
```

```python
import functools
import math

import jax
import jax.numpy as jnp
import numpy as np
from jax import lax
from jax.experimental import pallas as pl
from jax.experimental.pallas import tpu as pltpu
from jax.sharding import PartitionSpec as P

LMAX = 12
INNER = 0.5
COUPLING = 2000.0
LANES = 128
MESH = pl.DeviceIdType.MESH
SLOTS = [(l, k) for l in range(LMAX + 1) for k in range(2 * LMAX + 1) if (k + 1) // 2 <= l]
EVEN = [s for s in SLOTS if ((s[1] + 1) // 2) % 2 == 0]
ODD = [s for s in SLOTS if ((s[1] + 1) // 2) % 2 == 1]


def legendre_rows(total_rows):
    angle = (np.arange(total_rows) + 0.5) * (math.pi / total_rows)
    c, s = np.cos(angle), np.sin(angle)
    v = {(0, 0): np.full_like(angle, 1.0 / math.sqrt(4.0 * math.pi))}
    for m in range(1, LMAX + 1):
        v[m, m] = math.sqrt((2.0 * m + 1.0) / (2.0 * m)) * s * v[m - 1, m - 1]
    for m in range(LMAX):
        v[m + 1, m] = math.sqrt(2.0 * m + 3.0) * c * v[m, m]
    for m in range(LMAX + 1):
        for l in range(m + 2, LMAX + 1):
            a = math.sqrt((4.0 * l * l - 1.0) / (l * l - m * m))
            b = math.sqrt(((l - 1.0) ** 2 - m * m) / (4.0 * (l - 1.0) ** 2 - 1.0))
            v[l, m] = a * (c * v[l - 1, m] - b * v[l - 2, m])
    table = np.zeros((total_rows, 2 * LANES))
    for base, group in ((0, EVEN), (LANES, ODD)):
        for n, (l, k) in enumerate(group):
            table[:, base + n] = v[l, (k + 1) // 2]
    return table, s


def fourier_columns(phi_cells, group):
    phi = np.arange(phi_cells // 2) * (2.0 * math.pi / phi_cells)
    table = np.zeros((phi_cells // 2, LANES))
    for n, (_, k) in enumerate(group):
        m = (k + 1) // 2
        if k == 0:
            table[:, n] = 1.0
        else:
            table[:, n] = math.sqrt(2.0) * (np.cos(m * phi) if k % 2 else np.sin(m * phi))
    return table


def split_np(table):
    hi = np.asarray(table, np.float32).astype(jnp.bfloat16)
    lo = (table - hi.astype(np.float64)).astype(np.float32).astype(jnp.bfloat16)
    return hi, lo


def split(x):
    hi = x.astype(jnp.bfloat16)
    return hi, (x - hi.astype(jnp.float32)).astype(jnp.bfloat16)


class Packing:
    def __init__(self, owners, fields):
        half = owners // 2
        main = len(ODD)
        self.piece = -(-main // half)
        assert fields * self.piece <= LANES - 2 and fields <= owners
        self.moves = []
        for parity, count, base in ((0, half, 0), (1, owners - half, half)):
            for n in range(count):
                start = n * self.piece
                size = min(self.piece, main - start)
                if size > 0:
                    self.moves.append((base + n, parity, start, size))
        self.owners, self.fields = owners, fields
        self.last = len(EVEN) - 1
        self.spare = LANES - 2

    def degrees(self):
        table = np.zeros((-(-self.owners // 8) * 8, LANES), np.float32)
        for f in range(self.fields):
            for q, parity, start, size in self.moves:
                group = (EVEN, ODD)[parity]
                for n in range(size):
                    table[q, f * self.piece + n] = group[start + n][0]
            table[f, self.spare] = EVEN[self.last][0]
        return table

    def pack(self, tiles):
        lane = lax.broadcasted_iota(jnp.int32, tiles[0][0].shape, 1)
        out = [jnp.zeros_like(tiles[0][0]) for _ in range(self.owners)]
        for f in range(self.fields):
            for q, parity, start, size in self.moves:
                to = f * self.piece
                moved = pltpu.roll(tiles[f][parity], (to - start) % LANES, 1)
                out[q] = jnp.where((lane >= to) & (lane < to + size), moved, out[q])
            moved = pltpu.roll(tiles[f][0], (self.spare - self.last) % LANES, 1)
            out[f] = jnp.where(lane == self.spare, moved, out[f])
        return out

    def unpack(self, packed, f):
        lane = lax.broadcasted_iota(jnp.int32, packed[0].shape, 1)
        out = [jnp.zeros_like(packed[0]) for _ in range(2)]
        for q, parity, start, size in self.moves:
            moved = pltpu.roll(packed[q], (start - f * self.piece) % LANES, 1)
            out[parity] = jnp.where((lane >= start) & (lane < start + size), moved, out[parity])
        moved = pltpu.roll(packed[f], (self.last - self.spare) % LANES, 1)
        out[0] = jnp.where(lane == self.last, moved, out[0])
        return out


def moments_kernel(
    n_rad, n_ang, packing, group, density, even_w, odd_w, weighted, degrees, out,
    rows_buf, even_buf, odd_buf, leg_buf, part, landed, totals, totals_in, coef,
    load_sem, table_sem, part_send, part_recv, tot_send, tot_recv, coef_send, coef_recv,
):
    fields, shells, thetas, phis = density.shape
    groups = shells // group
    half = phis // 2
    rad, ang = lax.axis_index("rad"), lax.axis_index("ang")

    def load(g, f):
        return pltpu.make_async_copy(
            density.at[f, pl.ds(g * group, group)], rows_buf.at[g * fields + f],
            load_sem.at[g * fields + f],
        )

    tables = [
        pltpu.make_async_copy(even_w, even_buf, table_sem.at[0]),
        pltpu.make_async_copy(odd_w, odd_buf, table_sem.at[1]),
        pltpu.make_async_copy(weighted.at[pl.ds(ang * thetas, thetas)], leg_buf, table_sem.at[2]),
    ]
    for copy in tables:
        copy.start()
    for g in range(groups):
        for f in range(fields):
            load(g, f).start()

    barrier = pltpu.get_barrier_semaphore()
    for d in range(1, n_ang):
        pl.semaphore_signal(
            barrier, inc=1, device_id=(rad, lax.rem(ang + d, n_ang)), device_id_type=MESH
        )
    for d in range(1, n_rad):
        pl.semaphore_signal(
            barrier, inc=1, device_id=(lax.rem(rad + d, n_rad), ang), device_id_type=MESH
        )

    def send_part(g, d):
        q = lax.rem(ang + d, n_ang)
        at = pl.ds(pl.multiple_of(g * group, group), group)
        return pltpu.make_async_remote_copy(
            src_ref=part.at[q, at], dst_ref=landed.at[n_ang - 1 - d, at],
            send_sem=part_send.at[d - 1, g], recv_sem=part_recv.at[n_ang - 1 - d, g],
            device_id=(rad, q), device_id_type=MESH,
        )

    def recv_part(g, slot):
        at = pl.ds(pl.multiple_of(g * group, group), group)
        return pltpu.make_async_remote_copy(
            src_ref=part.at[0, at], dst_ref=landed.at[slot, at],
            send_sem=part_send.at[slot, g], recv_sem=part_recv.at[slot, g],
            device_id=(rad, lax.rem(ang + 1, n_ang)), device_id_type=MESH,
        )

    degree = degrees[pl.ds(ang, 1), :]
    total_shells = shells * n_rad
    spacing = (1.0 - INNER) / total_shells
    index = rad * shells + lax.broadcasted_iota(jnp.int32, (shells, LANES), 0)
    log_r = jnp.log(INNER + (index.astype(jnp.float32) + 0.5) * spacing)
    factor = (-COUPLING * 4.0 * math.pi) / (2.0 * degree + 1.0)
    inner_w = jnp.exp((degree + 2.0) * log_r) * spacing
    outer_w = jnp.exp((1.0 - degree) * log_r) * spacing
    inner_c = factor * jnp.exp(-(degree + 1.0) * log_r)
    outer_c = factor * jnp.exp(degree * log_r)

    for copy in tables:
        copy.wait()

    def one(g, _):
        tiles = []
        for f in range(fields):
            load(g, f).wait()
            x = rows_buf[g * fields + f].reshape(group * thetas, phis)
            left, right = x[:, :half], x[:, half:]
            pair = []
            for n, (v, w) in enumerate(((left + right, even_buf), (left - right, odd_buf))):
                hi, lo = split(v)
                both = jnp.dot(hi, w[...], preferred_element_type=jnp.float32)
                rest = jnp.dot(lo, w[:, :LANES], preferred_element_type=jnp.float32)
                az = both[:, :LANES] + both[:, LANES:] + rest
                az = az.reshape(group, thetas, LANES)
                az = az * leg_buf[:, n * LANES:(n + 1) * LANES][None]
                pair.append(jnp.sum(az, axis=1))
            tiles.append(pair)
        packed = packing.pack(tiles)
        at = pl.ds(pl.multiple_of(g * group, group), group)
        for q in range(n_ang):
            part[q, at, :] = packed[q]

        @pl.when(g == 0)
        def _():
            pl.semaphore_wait(barrier, n_ang + n_rad - 2)

        for d in range(1, n_ang):
            send_part(g, d).start()
        return 0

    lax.fori_loop(0, groups, one, 0)

    for g in range(groups):
        for slot in range(n_ang - 1):
            recv_part(g, slot).wait_recv()
    moments = part[ang]
    for slot in range(n_ang - 1):
        moments = moments + landed[slot]
    inner = moments * inner_w
    outer = moments * outer_w
    sub = lax.broadcasted_iota(jnp.int32, (8, LANES), 0)
    inner_total = jnp.sum(inner, axis=0, keepdims=True)
    outer_total = jnp.sum(outer, axis=0, keepdims=True)
    totals[...] = jnp.where(sub == 0, inner_total, jnp.where(sub == 1, outer_total, 0.0))

    def send_total(d):
        slot = n_rad - 1 - d
        return pltpu.make_async_remote_copy(
            src_ref=totals, dst_ref=totals_in.at[slot],
            send_sem=tot_send.at[d - 1], recv_sem=tot_recv.at[slot],
            device_id=(lax.rem(rad + d, n_rad), ang), device_id_type=MESH,
        )

    for d in range(1, n_rad):
        send_total(d).start()

    row = lax.broadcasted_iota(jnp.int32, (shells, shells), 0)
    col = lax.broadcasted_iota(jnp.int32, (shells, shells), 1)
    diag = jnp.where(row == col, 0.5, 0.0)
    below = jnp.where(col < row, 1.0, diag)
    above = jnp.where(col > row, 1.0, diag)
    inner_sum = jnp.dot(below, inner, precision=lax.Precision.HIGHEST, preferred_element_type=jnp.float32)
    outer_sum = jnp.dot(above, outer, precision=lax.Precision.HIGHEST, preferred_element_type=jnp.float32)

    from_below = jnp.zeros((1, LANES), jnp.float32)
    from_above = jnp.zeros((1, LANES), jnp.float32)
    for slot in range(n_rad - 1):
        send_total(n_rad - 1 - slot).wait_recv()
        source = lax.rem(rad + slot + 1, n_rad)
        got = totals_in[slot]
        from_below = from_below + jnp.where(source < rad, got[0:1], 0.0)
        from_above = from_above + jnp.where(source > rad, got[1:2], 0.0)
    coef[ang] = inner_c * (from_below + inner_sum) + outer_c * (from_above + outer_sum)

    def send_coef(d):
        return pltpu.make_async_remote_copy(
            src_ref=coef.at[ang], dst_ref=coef.at[ang],
            send_sem=coef_send.at[d - 1], recv_sem=coef_recv.at[n_ang - 1 - d],
            device_id=(rad, lax.rem(ang + d, n_ang)), device_id_type=MESH,
        )

    def recv_coef(d):
        q = lax.rem(ang + n_ang - d, n_ang)
        return pltpu.make_async_remote_copy(
            src_ref=coef.at[ang], dst_ref=coef.at[q],
            send_sem=coef_send.at[d - 1], recv_sem=coef_recv.at[n_ang - 1 - d],
            device_id=(rad, q), device_id_type=MESH,
        )

    for d in range(1, n_ang):
        send_coef(d).start()
    for d in range(1, n_ang):
        recv_coef(d).wait_recv()
    out[...] = coef[...]
    for d in range(1, n_ang):
        send_coef(d).wait_send()
        for g in range(groups):
            send_part(g, d).wait_send()
    for d in range(1, n_rad):
        send_total(d).wait_send()


def potential_kernel(packing, group, coef, legendre, even_w, odd_w, out, spread, rows_buf, store_sem):
    fields, shells, thetas, phis = out.shape
    groups = shells // group
    half = phis // 2
    first = pl.multiple_of(lax.axis_index("ang") * thetas, thetas)
    tiles = [coef[q] for q in range(packing.owners)]
    for f in range(fields):
        for parity, value in enumerate(packing.unpack(tiles, f)):
            spread[f, :, parity * LANES:(parity + 1) * LANES] = value

    def store(c):
        f, g = c // groups, c % groups
        return pltpu.make_async_copy(
            rows_buf.at[c], out.at[f, pl.ds(g * group, group)], store_sem.at[c]
        )

    def one(c, _):
        f, g = c // groups, c % groups
        sides = []
        for n, w in enumerate((even_w, odd_w)):
            lanes = slice(n * LANES, (n + 1) * LANES)
            c_rows = spread[f, pl.ds(pl.multiple_of(g * group, group), group), lanes]
            s = c_rows[:, None, :] * legendre[pl.ds(first, thetas), lanes][None]
            hi, lo = split(s.reshape(group * thetas, LANES))
            main = jnp.dot(
                jnp.concatenate([hi, lo], 1), w[: 2 * LANES], preferred_element_type=jnp.float32
            )
            rest = jnp.dot(hi, w[2 * LANES:], preferred_element_type=jnp.float32)
            sides.append(main + rest)
        rows_buf[c, :, :, :half] = (sides[0] + sides[1]).reshape(group, thetas, half)
        rows_buf[c, :, :, half:] = (sides[0] - sides[1]).reshape(group, thetas, half)
        store(c).start()
        return 0

    lax.fori_loop(0, fields * groups, one, 0)
    for c in range(fields * groups):
        store(c).wait()


def body(n_rad, n_ang, density):
    fields, shells, thetas, phis = density.shape
    group = math.gcd(shells, 16)
    groups = shells // group
    packing = Packing(n_ang, fields)
    total_rows = thetas * n_ang
    legendre, sine = legendre_rows(total_rows)
    weights = sine * (math.pi / total_rows) * (2.0 * math.pi / phis)
    weighted = jnp.asarray(legendre * weights[:, None], jnp.float32)
    forward, inverse = [], []
    for slots in (EVEN, ODD):
        table = fourier_columns(phis, slots)
        hi, lo = split_np(table)
        forward.append(jnp.asarray(np.concatenate([hi, lo], 1)))
        inverse.append(jnp.asarray(np.concatenate([hi.T, hi.T, lo.T], 0)))
    vmem = pl.BlockSpec(memory_space=pltpu.VMEM)
    anywhere = pl.BlockSpec(memory_space=pl.ANY)
    dma = pltpu.SemaphoreType.DMA
    coef = pl.pallas_call(
        functools.partial(moments_kernel, n_rad, n_ang, packing, group),
        out_shape=jax.ShapeDtypeStruct((n_ang, shells, LANES), jnp.float32),
        in_specs=[anywhere] * 4 + [vmem],
        out_specs=vmem,
        scratch_shapes=[
            pltpu.VMEM((fields * groups, group, thetas, phis), jnp.float32),
            pltpu.VMEM((phis // 2, 2 * LANES), jnp.bfloat16),
            pltpu.VMEM((phis // 2, 2 * LANES), jnp.bfloat16),
            pltpu.VMEM((thetas, 2 * LANES), jnp.float32),
            pltpu.VMEM((n_ang, shells, LANES), jnp.float32),
            pltpu.VMEM((n_ang - 1, shells, LANES), jnp.float32),
            pltpu.VMEM((8, LANES), jnp.float32),
            pltpu.VMEM((n_rad - 1, 8, LANES), jnp.float32),
            pltpu.VMEM((n_ang, shells, LANES), jnp.float32),
            dma((fields * groups,)),
            dma((3,)),
            dma((n_ang - 1, groups)),
            dma((n_ang - 1, groups)),
            dma((n_rad - 1,)),
            dma((n_rad - 1,)),
            dma((n_ang - 1,)),
            dma((n_ang - 1,)),
        ],
        compiler_params=pltpu.CompilerParams(collective_id=0, has_side_effects=True),
        name="moments",
    )(density, forward[0], forward[1], weighted, jnp.asarray(packing.degrees()))
    return pl.pallas_call(
        functools.partial(potential_kernel, packing, group),
        out_shape=jax.ShapeDtypeStruct(density.shape, jnp.float32),
        in_specs=[vmem] * 4,
        out_specs=anywhere,
        scratch_shapes=[
            pltpu.VMEM((fields, shells, 2 * LANES), jnp.float32),
            pltpu.VMEM((fields * groups, group, thetas, phis), jnp.float32),
            dma((fields * groups,)),
        ],
        name="potential",
    )(coef, jnp.asarray(legendre, jnp.float32), inverse[0], inverse[1])


def solution(mesh):
    sizes = mesh.shape
    return jax.shard_map(
        functools.partial(body, sizes["rad"], sizes["ang"]),
        mesh=mesh,
        in_specs=(P(None, "rad", "ang", None),),
        out_specs=P(None, "rad", "ang", None),
        check_vma=False,
    )
```

```python
import functools
import math

import jax
import jax.numpy as jnp
import numpy as np
from jax import lax
from jax.experimental import pallas as pl
from jax.experimental.pallas import tpu as pltpu
from jax.sharding import PartitionSpec as P

LMAX = 12
INNER = 0.5
COUPLING = 2000.0
LANES = 128
MESH = pl.DeviceIdType.MESH
SLOTS = [(l, k) for l in range(LMAX + 1) for k in range(2 * LMAX + 1) if (k + 1) // 2 <= l]
EVEN = [s for s in SLOTS if ((s[1] + 1) // 2) % 2 == 0]
ODD = [s for s in SLOTS if ((s[1] + 1) // 2) % 2 == 1]


def legendre_rows(total_rows):
    angle = (np.arange(total_rows) + 0.5) * (math.pi / total_rows)
    c, s = np.cos(angle), np.sin(angle)
    v = {(0, 0): np.full_like(angle, 1.0 / math.sqrt(4.0 * math.pi))}
    for m in range(1, LMAX + 1):
        v[m, m] = math.sqrt((2.0 * m + 1.0) / (2.0 * m)) * s * v[m - 1, m - 1]
    for m in range(LMAX):
        v[m + 1, m] = math.sqrt(2.0 * m + 3.0) * c * v[m, m]
    for m in range(LMAX + 1):
        for l in range(m + 2, LMAX + 1):
            a = math.sqrt((4.0 * l * l - 1.0) / (l * l - m * m))
            b = math.sqrt(((l - 1.0) ** 2 - m * m) / (4.0 * (l - 1.0) ** 2 - 1.0))
            v[l, m] = a * (c * v[l - 1, m] - b * v[l - 2, m])
    table = np.zeros((total_rows, 2 * LANES))
    for base, group in ((0, EVEN), (LANES, ODD)):
        for n, (l, k) in enumerate(group):
            table[:, base + n] = v[l, (k + 1) // 2]
    return table, s


def fourier_columns(phi_cells, group):
    phi = np.arange(phi_cells // 2) * (2.0 * math.pi / phi_cells)
    table = np.zeros((phi_cells // 2, LANES))
    for n, (_, k) in enumerate(group):
        m = (k + 1) // 2
        if k == 0:
            table[:, n] = 1.0
        else:
            table[:, n] = math.sqrt(2.0) * (np.cos(m * phi) if k % 2 else np.sin(m * phi))
    return table


def split_np(table):
    hi = np.asarray(table, np.float32).astype(jnp.bfloat16)
    lo = (table - hi.astype(np.float64)).astype(np.float32).astype(jnp.bfloat16)
    return hi, lo


def split(x):
    hi = x.astype(jnp.bfloat16)
    return hi, (x - hi.astype(jnp.float32)).astype(jnp.bfloat16)


class Packing:
    def __init__(self, owners, fields):
        half = owners // 2
        main = len(ODD)
        self.piece = -(-main // half)
        assert fields * self.piece <= LANES - 2 and fields <= owners
        self.moves = []
        for parity, count, base in ((0, half, 0), (1, owners - half, half)):
            for n in range(count):
                start = n * self.piece
                size = min(self.piece, main - start)
                if size > 0:
                    self.moves.append((base + n, parity, start, size))
        self.owners, self.fields = owners, fields
        self.last = len(EVEN) - 1
        self.spare = LANES - 2

    def degrees(self):
        table = np.zeros((-(-self.owners // 8) * 8, LANES), np.float32)
        for f in range(self.fields):
            for q, parity, start, size in self.moves:
                group = (EVEN, ODD)[parity]
                for n in range(size):
                    table[q, f * self.piece + n] = group[start + n][0]
            table[f, self.spare] = EVEN[self.last][0]
        return table

    def pack(self, tiles):
        lane = lax.broadcasted_iota(jnp.int32, tiles[0][0].shape, 1)
        out = [jnp.zeros_like(tiles[0][0]) for _ in range(self.owners)]
        for f in range(self.fields):
            for q, parity, start, size in self.moves:
                to = f * self.piece
                moved = pltpu.roll(tiles[f][parity], (to - start) % LANES, 1)
                out[q] = jnp.where((lane >= to) & (lane < to + size), moved, out[q])
            moved = pltpu.roll(tiles[f][0], (self.spare - self.last) % LANES, 1)
            out[f] = jnp.where(lane == self.spare, moved, out[f])
        return out

    def unpack(self, packed, f):
        lane = lax.broadcasted_iota(jnp.int32, packed[0].shape, 1)
        out = [jnp.zeros_like(packed[0]) for _ in range(2)]
        for q, parity, start, size in self.moves:
            moved = pltpu.roll(packed[q], (start - f * self.piece) % LANES, 1)
            out[parity] = jnp.where((lane >= start) & (lane < start + size), moved, out[parity])
        moved = pltpu.roll(packed[f], (self.last - self.spare) % LANES, 1)
        out[0] = jnp.where(lane == self.last, moved, out[0])
        return out


def moments_kernel(
    n_rad, n_ang, packing, group, density, even_w, odd_w, weighted, degrees, out,
    rows_buf, even_buf, odd_buf, leg_buf, part, landed, totals, totals_in, coef, powers,
    load_sem, table_sem, part_send, part_recv, tot_send, tot_recv, coef_send, coef_recv,
):
    fields, shells, thetas, phis = density.shape
    groups = shells // group
    half = phis // 2
    rad, ang = lax.axis_index("rad"), lax.axis_index("ang")

    def load(g, f):
        return pltpu.make_async_copy(
            density.at[f, pl.ds(g * group, group)], rows_buf.at[g * fields + f],
            load_sem.at[g * fields + f],
        )

    tables = [
        pltpu.make_async_copy(even_w, even_buf, table_sem.at[0]),
        pltpu.make_async_copy(odd_w, odd_buf, table_sem.at[1]),
        pltpu.make_async_copy(weighted.at[pl.ds(ang * thetas, thetas)], leg_buf, table_sem.at[2]),
    ]
    for copy in tables:
        copy.start()
    ahead = min(2, groups * fields)
    for c in range(ahead):
        load(c // fields, c % fields).start()

    barrier = pltpu.get_barrier_semaphore()
    for d in range(1, n_ang):
        pl.semaphore_signal(
            barrier, inc=1, device_id=(rad, lax.rem(ang + d, n_ang)), device_id_type=MESH
        )
    for d in range(1, n_rad):
        for z in range(n_ang):
            pl.semaphore_signal(
                barrier, inc=1, device_id=(lax.rem(rad + d, n_rad), lax.rem(ang + z, n_ang)),
                device_id_type=MESH,
            )

    def send_part(g, d):
        q = lax.rem(ang + d, n_ang)
        at = pl.ds(pl.multiple_of(g * group, group), group)
        return pltpu.make_async_remote_copy(
            src_ref=part.at[q, at], dst_ref=landed.at[n_ang - 1 - d, at],
            send_sem=part_send.at[d - 1, g], recv_sem=part_recv.at[n_ang - 1 - d, g],
            device_id=(rad, q), device_id_type=MESH,
        )

    def recv_part(g, slot):
        at = pl.ds(pl.multiple_of(g * group, group), group)
        return pltpu.make_async_remote_copy(
            src_ref=part.at[0, at], dst_ref=landed.at[slot, at],
            send_sem=part_send.at[slot, g], recv_sem=part_recv.at[slot, g],
            device_id=(rad, lax.rem(ang + 1, n_ang)), device_id_type=MESH,
        )

    degree = degrees[pl.ds(ang, 1), :]
    total_shells = shells * n_rad
    spacing = (1.0 - INNER) / total_shells
    index = rad * shells + lax.broadcasted_iota(jnp.int32, (shells, LANES), 0)
    log_r = jnp.log(INNER + (index.astype(jnp.float32) + 0.5) * spacing)
    factor = (-COUPLING * 4.0 * math.pi) / (2.0 * degree + 1.0)
    for q in range(n_ang):
        powers[0, q] = jnp.exp((degrees[q:q + 1, :] + 2.0) * log_r) * spacing
        powers[1, q] = jnp.exp((1.0 - degrees[q:q + 1, :]) * log_r) * spacing
    inner_c = factor * jnp.exp(-(degree + 1.0) * log_r)
    outer_c = factor * jnp.exp(degree * log_r)

    for copy in tables:
        copy.wait()

    def one(g, _):
        tiles = []
        for f in range(fields):
            load(g, f).wait()
            c = g * fields + f + ahead

            @pl.when(c < groups * fields)
            def _():
                load(c // fields, c % fields).start()

            x = rows_buf[g * fields + f].reshape(group * thetas, phis)
            left, right = x[:, :half], x[:, half:]
            pair = []
            for n, (v, w) in enumerate(((left + right, even_buf), (left - right, odd_buf))):
                hi, lo = split(v)
                both = jnp.dot(hi, w[...], preferred_element_type=jnp.float32)
                rest = jnp.dot(lo, w[:, :LANES], preferred_element_type=jnp.float32)
                az = both[:, :LANES] + both[:, LANES:] + rest
                az = az.reshape(group, thetas, LANES)
                az = az * leg_buf[:, n * LANES:(n + 1) * LANES][None]
                pair.append(jnp.sum(az, axis=1))
            tiles.append(pair)
        packed = packing.pack(tiles)
        at = pl.ds(pl.multiple_of(g * group, group), group)
        for q in range(n_ang):
            part[q, at, :] = packed[q]

        @pl.when(g == 0)
        def _():
            pl.semaphore_wait(barrier, n_ang * n_rad - 1)

        for d in range(1, n_ang):
            send_part(g, d).start()
        return 0

    lax.fori_loop(0, groups, one, 0)

    sub = lax.broadcasted_iota(jnp.int32, (8, LANES), 0)
    for q in range(n_ang):
        inner_total = jnp.sum(part[q] * powers[0, q], axis=0, keepdims=True)
        outer_total = jnp.sum(part[q] * powers[1, q], axis=0, keepdims=True)
        totals[q] = jnp.where(sub == 0, inner_total, jnp.where(sub == 1, outer_total, 0.0))

    def send_total(d, z):
        slot = n_rad - 1 - d
        q = lax.rem(ang + z, n_ang)
        return pltpu.make_async_remote_copy(
            src_ref=totals.at[q], dst_ref=totals_in.at[slot, z],
            send_sem=tot_send.at[d - 1, z], recv_sem=tot_recv.at[slot, z],
            device_id=(lax.rem(rad + d, n_rad), q), device_id_type=MESH,
        )

    for z in [*range(1, n_ang), 0]:
        for d in range(1, n_rad):
            send_total(d, z).start()

    for g in range(groups):
        for slot in range(n_ang - 1):
            recv_part(g, slot).wait_recv()
    moments = part[ang]
    for slot in range(n_ang - 1):
        moments = moments + landed[slot]
    inner = moments * powers[0, ang]
    outer = moments * powers[1, ang]
    row = lax.broadcasted_iota(jnp.int32, (shells, shells), 0)
    col = lax.broadcasted_iota(jnp.int32, (shells, shells), 1)
    diag = jnp.where(row == col, 0.5, 0.0)
    below = jnp.where(col < row, 1.0, diag)
    above = jnp.where(col > row, 1.0, diag)
    inner_sum = jnp.dot(below, inner, precision=lax.Precision.HIGHEST, preferred_element_type=jnp.float32)
    outer_sum = jnp.dot(above, outer, precision=lax.Precision.HIGHEST, preferred_element_type=jnp.float32)

    from_below = jnp.zeros((8, LANES), jnp.float32)
    from_above = jnp.zeros((8, LANES), jnp.float32)
    for slot in range(n_rad - 1):
        got = jnp.zeros((8, LANES), jnp.float32)
        for z in range(n_ang):
            send_total(n_rad - 1 - slot, z).wait_recv()
            got = got + totals_in[slot, z]
        source = lax.rem(rad + slot + 1, n_rad)
        from_below = from_below + jnp.where(source < rad, got, 0.0)
        from_above = from_above + jnp.where(source > rad, got, 0.0)
    coef[ang] = inner_c * (from_below[0:1] + inner_sum) + outer_c * (
        from_above[1:2] + outer_sum
    )

    def send_coef(d):
        return pltpu.make_async_remote_copy(
            src_ref=coef.at[ang], dst_ref=coef.at[ang],
            send_sem=coef_send.at[d - 1], recv_sem=coef_recv.at[n_ang - 1 - d],
            device_id=(rad, lax.rem(ang + d, n_ang)), device_id_type=MESH,
        )

    def recv_coef(d):
        q = lax.rem(ang + n_ang - d, n_ang)
        return pltpu.make_async_remote_copy(
            src_ref=coef.at[ang], dst_ref=coef.at[q],
            send_sem=coef_send.at[d - 1], recv_sem=coef_recv.at[n_ang - 1 - d],
            device_id=(rad, q), device_id_type=MESH,
        )

    for d in range(1, n_ang):
        send_coef(d).start()
    for d in range(1, n_ang):
        recv_coef(d).wait_recv()
    out[...] = coef[...]
    for d in range(1, n_ang):
        send_coef(d).wait_send()
        for g in range(groups):
            send_part(g, d).wait_send()
    for d in range(1, n_rad):
        for z in range(n_ang):
            send_total(d, z).wait_send()


def potential_kernel(packing, group, coef, legendre, even_w, odd_w, out, spread, rows_buf, store_sem):
    fields, shells, thetas, phis = out.shape
    groups = shells // group
    half = phis // 2
    first = pl.multiple_of(lax.axis_index("ang") * thetas, thetas)
    tiles = [coef[q] for q in range(packing.owners)]
    for f in range(fields):
        for parity, value in enumerate(packing.unpack(tiles, f)):
            spread[f, :, parity * LANES:(parity + 1) * LANES] = value

    def store(c):
        f, g = c // groups, c % groups
        return pltpu.make_async_copy(
            rows_buf.at[c], out.at[f, pl.ds(g * group, group)], store_sem.at[c]
        )

    def one(c, _):
        f, g = c // groups, c % groups
        sides = []
        for n, w in enumerate((even_w, odd_w)):
            lanes = slice(n * LANES, (n + 1) * LANES)
            c_rows = spread[f, pl.ds(pl.multiple_of(g * group, group), group), lanes]
            s = c_rows[:, None, :] * legendre[pl.ds(first, thetas), lanes][None]
            hi, lo = split(s.reshape(group * thetas, LANES))
            main = jnp.dot(
                jnp.concatenate([hi, lo], 1), w[: 2 * LANES], preferred_element_type=jnp.float32
            )
            rest = jnp.dot(hi, w[2 * LANES:], preferred_element_type=jnp.float32)
            sides.append(main + rest)
        rows_buf[c, :, :, :half] = (sides[0] + sides[1]).reshape(group, thetas, half)
        rows_buf[c, :, :, half:] = (sides[0] - sides[1]).reshape(group, thetas, half)
        store(c).start()
        return 0

    lax.fori_loop(0, fields * groups, one, 0)
    for c in range(fields * groups):
        store(c).wait()


def body(n_rad, n_ang, density):
    fields, shells, thetas, phis = density.shape
    group = math.gcd(shells, 32)
    groups = shells // group
    packing = Packing(n_ang, fields)
    total_rows = thetas * n_ang
    legendre, sine = legendre_rows(total_rows)
    weights = sine * (math.pi / total_rows) * (2.0 * math.pi / phis)
    weighted = jnp.asarray(legendre * weights[:, None], jnp.float32)
    forward, inverse = [], []
    for slots in (EVEN, ODD):
        table = fourier_columns(phis, slots)
        hi, lo = split_np(table)
        forward.append(jnp.asarray(np.concatenate([hi, lo], 1)))
        inverse.append(jnp.asarray(np.concatenate([hi.T, hi.T, lo.T], 0)))
    vmem = pl.BlockSpec(memory_space=pltpu.VMEM)
    anywhere = pl.BlockSpec(memory_space=pl.ANY)
    dma = pltpu.SemaphoreType.DMA
    coef = pl.pallas_call(
        functools.partial(moments_kernel, n_rad, n_ang, packing, group),
        out_shape=jax.ShapeDtypeStruct((n_ang, shells, LANES), jnp.float32),
        in_specs=[anywhere] * 4 + [vmem],
        out_specs=vmem,
        scratch_shapes=[
            pltpu.VMEM((fields * groups, group, thetas, phis), jnp.float32),
            pltpu.VMEM((phis // 2, 2 * LANES), jnp.bfloat16),
            pltpu.VMEM((phis // 2, 2 * LANES), jnp.bfloat16),
            pltpu.VMEM((thetas, 2 * LANES), jnp.float32),
            pltpu.VMEM((n_ang, shells, LANES), jnp.float32),
            pltpu.VMEM((n_ang - 1, shells, LANES), jnp.float32),
            pltpu.VMEM((n_ang, 8, LANES), jnp.float32),
            pltpu.VMEM((n_rad - 1, n_ang, 8, LANES), jnp.float32),
            pltpu.VMEM((n_ang, shells, LANES), jnp.float32),
            pltpu.VMEM((2, n_ang, shells, LANES), jnp.float32),
            dma((fields * groups,)),
            dma((3,)),
            dma((n_ang - 1, groups)),
            dma((n_ang - 1, groups)),
            dma((n_rad - 1, n_ang)),
            dma((n_rad - 1, n_ang)),
            dma((n_ang - 1,)),
            dma((n_ang - 1,)),
        ],
        compiler_params=pltpu.CompilerParams(collective_id=0, has_side_effects=True),
        name="moments",
    )(density, forward[0], forward[1], weighted, jnp.asarray(packing.degrees()))
    return pl.pallas_call(
        functools.partial(potential_kernel, packing, group),
        out_shape=jax.ShapeDtypeStruct(density.shape, jnp.float32),
        in_specs=[vmem] * 4,
        out_specs=anywhere,
        scratch_shapes=[
            pltpu.VMEM((fields, shells, 2 * LANES), jnp.float32),
            pltpu.VMEM((fields * groups, group, thetas, phis), jnp.float32),
            dma((fields * groups,)),
        ],
        name="potential",
    )(coef, jnp.asarray(legendre, jnp.float32), inverse[0], inverse[1])


def solution(mesh):
    sizes = mesh.shape
    return jax.shard_map(
        functools.partial(body, sizes["rad"], sizes["ang"]),
        mesh=mesh,
        in_specs=(P(None, "rad", "ang", None),),
        out_specs=P(None, "rad", "ang", None),
        check_vma=False,
    )
```

```python
import functools
import math

import jax
import jax.numpy as jnp
import numpy as np
from jax import lax
from jax.experimental import pallas as pl
from jax.experimental.pallas import tpu as pltpu
from jax.sharding import PartitionSpec as P

LMAX = 12
INNER = 0.5
COUPLING = 2000.0
LANES = 128
MESH = pl.DeviceIdType.MESH
SLOTS = [(l, k) for l in range(LMAX + 1) for k in range(2 * LMAX + 1) if (k + 1) // 2 <= l]
EVEN = [s for s in SLOTS if ((s[1] + 1) // 2) % 2 == 0]
ODD = [s for s in SLOTS if ((s[1] + 1) // 2) % 2 == 1]


def legendre_rows(total_rows):
    angle = (np.arange(total_rows) + 0.5) * (math.pi / total_rows)
    c, s = np.cos(angle), np.sin(angle)
    v = {(0, 0): np.full_like(angle, 1.0 / math.sqrt(4.0 * math.pi))}
    for m in range(1, LMAX + 1):
        v[m, m] = math.sqrt((2.0 * m + 1.0) / (2.0 * m)) * s * v[m - 1, m - 1]
    for m in range(LMAX):
        v[m + 1, m] = math.sqrt(2.0 * m + 3.0) * c * v[m, m]
    for m in range(LMAX + 1):
        for l in range(m + 2, LMAX + 1):
            a = math.sqrt((4.0 * l * l - 1.0) / (l * l - m * m))
            b = math.sqrt(((l - 1.0) ** 2 - m * m) / (4.0 * (l - 1.0) ** 2 - 1.0))
            v[l, m] = a * (c * v[l - 1, m] - b * v[l - 2, m])
    table = np.zeros((total_rows, 2 * LANES))
    for base, group in ((0, EVEN), (LANES, ODD)):
        for n, (l, k) in enumerate(group):
            table[:, base + n] = v[l, (k + 1) // 2]
    return table, s


def fourier_columns(phi_cells, group):
    phi = np.arange(phi_cells // 2) * (2.0 * math.pi / phi_cells)
    table = np.zeros((phi_cells // 2, LANES))
    for n, (_, k) in enumerate(group):
        m = (k + 1) // 2
        if k == 0:
            table[:, n] = 1.0
        else:
            table[:, n] = math.sqrt(2.0) * (np.cos(m * phi) if k % 2 else np.sin(m * phi))
    return table


def split_np(table):
    hi = np.asarray(table, np.float32).astype(jnp.bfloat16)
    lo = (table - hi.astype(np.float64)).astype(np.float32).astype(jnp.bfloat16)
    return hi, lo


def split(x):
    hi = x.astype(jnp.bfloat16)
    return hi, (x - hi.astype(jnp.float32)).astype(jnp.bfloat16)


class Packing:
    def __init__(self, owners, fields):
        half = owners // 2
        main = len(ODD)
        self.piece = -(-main // half)
        assert fields * self.piece <= LANES - 2 and fields <= owners
        self.moves = []
        for parity, count, base in ((0, half, 0), (1, owners - half, half)):
            for n in range(count):
                start = n * self.piece
                size = min(self.piece, main - start)
                if size > 0:
                    self.moves.append((base + n, parity, start, size))
        self.owners, self.fields = owners, fields
        self.last = len(EVEN) - 1
        self.spare = LANES - 2

    def degrees(self):
        table = np.zeros((-(-self.owners // 8) * 8, LANES), np.float32)
        for f in range(self.fields):
            for q, parity, start, size in self.moves:
                group = (EVEN, ODD)[parity]
                for n in range(size):
                    table[q, f * self.piece + n] = group[start + n][0]
            table[f, self.spare] = EVEN[self.last][0]
        return table

    def pack(self, tiles):
        lane = lax.broadcasted_iota(jnp.int32, tiles[0][0].shape, 1)
        out = [jnp.zeros_like(tiles[0][0]) for _ in range(self.owners)]
        for f in range(self.fields):
            for q, parity, start, size in self.moves:
                to = f * self.piece
                moved = pltpu.roll(tiles[f][parity], (to - start) % LANES, 1)
                out[q] = jnp.where((lane >= to) & (lane < to + size), moved, out[q])
            moved = pltpu.roll(tiles[f][0], (self.spare - self.last) % LANES, 1)
            out[f] = jnp.where(lane == self.spare, moved, out[f])
        return out

    def unpack(self, packed, f):
        lane = lax.broadcasted_iota(jnp.int32, packed[0].shape, 1)
        out = [jnp.zeros_like(packed[0]) for _ in range(2)]
        for q, parity, start, size in self.moves:
            moved = pltpu.roll(packed[q], (start - f * self.piece) % LANES, 1)
            out[parity] = jnp.where((lane >= start) & (lane < start + size), moved, out[parity])
        moved = pltpu.roll(packed[f], (self.last - self.spare) % LANES, 1)
        out[0] = jnp.where(lane == self.last, moved, out[0])
        return out


def moments_kernel(
    n_rad, n_ang, packing, group, density, table, out,
    rows_buf, even_buf, odd_buf, part, landed, totals, totals_in, coef, powers,
    load_sem, part_send, part_recv, tot_send, tot_recv, coef_send, coef_recv,
):
    fields, shells, thetas, phis = density.shape
    groups = shells // group
    half = phis // 2
    rad, ang = lax.axis_index("rad"), lax.axis_index("ang")

    def load(g, f):
        return pltpu.make_async_copy(
            density.at[f, pl.ds(g * group, group)], rows_buf.at[g * fields + f],
            load_sem.at[g * fields + f],
        )

    ahead = min(2, groups * fields)
    for c in range(ahead):
        load(c // fields, c % fields).start()

    barrier = pltpu.get_barrier_semaphore()
    for d in range(1, n_ang):
        pl.semaphore_signal(
            barrier, inc=1, device_id=(rad, lax.rem(ang + d, n_ang)), device_id_type=MESH
        )
    for d in range(1, n_rad):
        for z in range(n_ang):
            pl.semaphore_signal(
                barrier, inc=1, device_id=(lax.rem(rad + d, n_rad), lax.rem(ang + z, n_ang)),
                device_id_type=MESH,
            )

    def send_part(g, d):
        q = lax.rem(ang + d, n_ang)
        at = pl.ds(pl.multiple_of(g * group, group), group)
        return pltpu.make_async_remote_copy(
            src_ref=part.at[q, at], dst_ref=landed.at[n_ang - 1 - d, at],
            send_sem=part_send.at[d - 1, g], recv_sem=part_recv.at[n_ang - 1 - d, g],
            device_id=(rad, q), device_id_type=MESH,
        )

    def recv_part(g, slot):
        at = pl.ds(pl.multiple_of(g * group, group), group)
        return pltpu.make_async_remote_copy(
            src_ref=part.at[0, at], dst_ref=landed.at[slot, at],
            send_sem=part_send.at[slot, g], recv_sem=part_recv.at[slot, g],
            device_id=(rad, lax.rem(ang + 1, n_ang)), device_id_type=MESH,
        )

    degrees = table[phis + n_ang * thetas:, :LANES]

    degree = degrees[0:1]
    for q in range(1, n_ang):
        degree = jnp.where(ang == q, degrees[q:q + 1], degree)
    total_shells = shells * n_rad
    spacing = (1.0 - INNER) / total_shells
    index = rad * shells + lax.broadcasted_iota(jnp.int32, (shells, LANES), 0)
    log_r = jnp.log(INNER + (index.astype(jnp.float32) + 0.5) * spacing)
    factor = (-COUPLING * 4.0 * math.pi) / (2.0 * degree + 1.0)
    for q in range(n_ang):
        powers[0, q] = jnp.exp((degrees[q:q + 1, :] + 2.0) * log_r) * spacing
        powers[1, q] = jnp.exp((1.0 - degrees[q:q + 1, :]) * log_r) * spacing
    inner_c = factor * jnp.exp(-(degree + 1.0) * log_r)
    outer_c = factor * jnp.exp(degree * log_r)

    even_buf[...] = table[:half].astype(jnp.bfloat16)
    odd_buf[...] = table[half:phis].astype(jnp.bfloat16)
    leg_at = pl.ds(pl.multiple_of(phis + ang * thetas, thetas), thetas)

    def one(g, _):
        tiles = []
        for f in range(fields):
            load(g, f).wait()
            c = g * fields + f + ahead

            @pl.when(c < groups * fields)
            def _():
                load(c // fields, c % fields).start()

            x = rows_buf[g * fields + f].reshape(group * thetas, phis)
            left, right = x[:, :half], x[:, half:]
            pair = []
            for n, (v, w) in enumerate(((left + right, even_buf), (left - right, odd_buf))):
                hi, lo = split(v)
                both = jnp.dot(hi, w[...], preferred_element_type=jnp.float32)
                rest = jnp.dot(lo, w[:, :LANES], preferred_element_type=jnp.float32)
                az = both[:, :LANES] + both[:, LANES:] + rest
                az = az.reshape(group, thetas, LANES)
                az = az * table[leg_at, n * LANES:(n + 1) * LANES][None]
                pair.append(jnp.sum(az, axis=1))
            tiles.append(pair)
        packed = packing.pack(tiles)
        at = pl.ds(pl.multiple_of(g * group, group), group)
        for q in range(n_ang):
            part[q, at, :] = packed[q]

        @pl.when(g == 0)
        def _():
            pl.semaphore_wait(barrier, n_ang * n_rad - 1)

        for d in range(1, n_ang):
            send_part(g, d).start()
        return 0

    lax.fori_loop(0, groups, one, 0)

    sub = lax.broadcasted_iota(jnp.int32, (8, LANES), 0)
    for q in range(n_ang):
        inner_total = jnp.sum(part[q] * powers[0, q], axis=0, keepdims=True)
        outer_total = jnp.sum(part[q] * powers[1, q], axis=0, keepdims=True)
        totals[q] = jnp.where(sub == 0, inner_total, jnp.where(sub == 1, outer_total, 0.0))

    def send_total(d, z):
        slot = n_rad - 1 - d
        q = lax.rem(ang + z, n_ang)
        return pltpu.make_async_remote_copy(
            src_ref=totals.at[q], dst_ref=totals_in.at[slot, z],
            send_sem=tot_send.at[d - 1, z], recv_sem=tot_recv.at[slot, z],
            device_id=(lax.rem(rad + d, n_rad), q), device_id_type=MESH,
        )

    for z in [*range(1, n_ang), 0]:
        for d in range(1, n_rad):
            send_total(d, z).start()

    for g in range(groups):
        for slot in range(n_ang - 1):
            recv_part(g, slot).wait_recv()
    moments = part[ang]
    for slot in range(n_ang - 1):
        moments = moments + landed[slot]
    inner = moments * powers[0, ang]
    outer = moments * powers[1, ang]
    row = lax.broadcasted_iota(jnp.int32, (shells, shells), 0)
    col = lax.broadcasted_iota(jnp.int32, (shells, shells), 1)
    diag = jnp.where(row == col, 0.5, 0.0)
    below = jnp.where(col < row, 1.0, diag)
    above = jnp.where(col > row, 1.0, diag)
    inner_sum = jnp.dot(below, inner, precision=lax.Precision.HIGHEST, preferred_element_type=jnp.float32)
    outer_sum = jnp.dot(above, outer, precision=lax.Precision.HIGHEST, preferred_element_type=jnp.float32)

    from_below = jnp.zeros((8, LANES), jnp.float32)
    from_above = jnp.zeros((8, LANES), jnp.float32)
    for slot in range(n_rad - 1):
        got = jnp.zeros((8, LANES), jnp.float32)
        for z in range(n_ang):
            send_total(n_rad - 1 - slot, z).wait_recv()
            got = got + totals_in[slot, z]
        source = lax.rem(rad + slot + 1, n_rad)
        from_below = from_below + jnp.where(source < rad, got, 0.0)
        from_above = from_above + jnp.where(source > rad, got, 0.0)
    coef[ang] = inner_c * (from_below[0:1] + inner_sum) + outer_c * (
        from_above[1:2] + outer_sum
    )

    def send_coef(d):
        return pltpu.make_async_remote_copy(
            src_ref=coef.at[ang], dst_ref=coef.at[ang],
            send_sem=coef_send.at[d - 1], recv_sem=coef_recv.at[n_ang - 1 - d],
            device_id=(rad, lax.rem(ang + d, n_ang)), device_id_type=MESH,
        )

    def recv_coef(d):
        q = lax.rem(ang + n_ang - d, n_ang)
        return pltpu.make_async_remote_copy(
            src_ref=coef.at[ang], dst_ref=coef.at[q],
            send_sem=coef_send.at[d - 1], recv_sem=coef_recv.at[n_ang - 1 - d],
            device_id=(rad, q), device_id_type=MESH,
        )

    for d in range(1, n_ang):
        send_coef(d).start()
    for d in range(1, n_ang):
        recv_coef(d).wait_recv()
    out[...] = coef[...]
    for d in range(1, n_ang):
        send_coef(d).wait_send()
        for g in range(groups):
            send_part(g, d).wait_send()
    for d in range(1, n_rad):
        for z in range(n_ang):
            send_total(d, z).wait_send()


def potential_kernel(packing, group, coef, legendre, even_w, odd_w, out, spread, rows_buf, store_sem):
    fields, shells, thetas, phis = out.shape
    groups = shells // group
    half = phis // 2
    first = pl.multiple_of(lax.axis_index("ang") * thetas, thetas)
    tiles = [coef[q] for q in range(packing.owners)]
    for f in range(fields):
        for parity, value in enumerate(packing.unpack(tiles, f)):
            spread[f, :, parity * LANES:(parity + 1) * LANES] = value

    def store(c):
        f, g = c // groups, c % groups
        return pltpu.make_async_copy(
            rows_buf.at[c], out.at[f, pl.ds(g * group, group)], store_sem.at[c]
        )

    def one(c, _):
        f, g = c // groups, c % groups
        sides = []
        for n, w in enumerate((even_w, odd_w)):
            lanes = slice(n * LANES, (n + 1) * LANES)
            c_rows = spread[f, pl.ds(pl.multiple_of(g * group, group), group), lanes]
            s = c_rows[:, None, :] * legendre[pl.ds(first, thetas), lanes][None]
            hi, lo = split(s.reshape(group * thetas, LANES))
            main = jnp.dot(
                jnp.concatenate([hi, lo], 1), w[: 2 * LANES], preferred_element_type=jnp.float32
            )
            rest = jnp.dot(hi, w[2 * LANES:], preferred_element_type=jnp.float32)
            sides.append(main + rest)
        rows_buf[c, :, :, :half] = (sides[0] + sides[1]).reshape(group, thetas, half)
        rows_buf[c, :, :, half:] = (sides[0] - sides[1]).reshape(group, thetas, half)
        store(c).start()
        return 0

    lax.fori_loop(0, fields * groups, one, 0)
    for c in range(fields * groups):
        store(c).wait()


def body(n_rad, n_ang, density):
    fields, shells, thetas, phis = density.shape
    group = math.gcd(shells, 32)
    groups = shells // group
    packing = Packing(n_ang, fields)
    total_rows = thetas * n_ang
    legendre, sine = legendre_rows(total_rows)
    weights = sine * (math.pi / total_rows) * (2.0 * math.pi / phis)
    weighted = np.asarray(legendre * weights[:, None], np.float32)
    forward, inverse = [], []
    for slots in (EVEN, ODD):
        table = fourier_columns(phis, slots)
        hi, lo = split_np(table)
        forward.append(np.concatenate([hi, lo], 1).astype(np.float32))
        inverse.append(jnp.asarray(np.concatenate([hi.T, hi.T, lo.T], 0)))
    degrees = np.tile(packing.degrees(), (1, 2))
    table = jnp.asarray(np.concatenate([*forward, weighted, degrees], 0))
    vmem = pl.BlockSpec(memory_space=pltpu.VMEM)
    anywhere = pl.BlockSpec(memory_space=pl.ANY)
    dma = pltpu.SemaphoreType.DMA
    coef = pl.pallas_call(
        functools.partial(moments_kernel, n_rad, n_ang, packing, group),
        out_shape=jax.ShapeDtypeStruct((n_ang, shells, LANES), jnp.float32),
        in_specs=[anywhere, vmem],
        out_specs=vmem,
        scratch_shapes=[
            pltpu.VMEM((fields * groups, group, thetas, phis), jnp.float32),
            pltpu.VMEM((phis // 2, 2 * LANES), jnp.bfloat16),
            pltpu.VMEM((phis // 2, 2 * LANES), jnp.bfloat16),
            pltpu.VMEM((n_ang, shells, LANES), jnp.float32),
            pltpu.VMEM((n_ang - 1, shells, LANES), jnp.float32),
            pltpu.VMEM((n_ang, 8, LANES), jnp.float32),
            pltpu.VMEM((n_rad - 1, n_ang, 8, LANES), jnp.float32),
            pltpu.VMEM((n_ang, shells, LANES), jnp.float32),
            pltpu.VMEM((2, n_ang, shells, LANES), jnp.float32),
            dma((fields * groups,)),
            dma((n_ang - 1, groups)),
            dma((n_ang - 1, groups)),
            dma((n_rad - 1, n_ang)),
            dma((n_rad - 1, n_ang)),
            dma((n_ang - 1,)),
            dma((n_ang - 1,)),
        ],
        compiler_params=pltpu.CompilerParams(collective_id=0, has_side_effects=True, vmem_limit_bytes=52 << 20),
        name="moments",
    )(density, table)
    return pl.pallas_call(
        functools.partial(potential_kernel, packing, group),
        out_shape=jax.ShapeDtypeStruct(density.shape, jnp.float32),
        in_specs=[vmem] * 4,
        out_specs=anywhere,
        scratch_shapes=[
            pltpu.VMEM((fields, shells, 2 * LANES), jnp.float32),
            pltpu.VMEM((fields * groups, group, thetas, phis), jnp.float32),
            dma((fields * groups,)),
        ],
        compiler_params=pltpu.CompilerParams(vmem_limit_bytes=52 << 20),
        name="potential",
    )(coef, jnp.asarray(legendre, jnp.float32), inverse[0], inverse[1])


def solution(mesh):
    sizes = mesh.shape
    return jax.shard_map(
        functools.partial(body, sizes["rad"], sizes["ang"]),
        mesh=mesh,
        in_specs=(P(None, "rad", "ang", None),),
        out_specs=P(None, "rad", "ang", None),
        check_vma=False,
    )
```
